16 devices in a mesh: dp: 4 (over y, z, core), tp: 4 (over x).
Axes of the slice: x: 4, y: 2, z: 1, core: 2. Of those that a mesh axis runs over, the one named last changes fastest.
The devices are a block of a 4x4x4 slice.
Arguments:
- x: bfloat16 [3072, 6144], P(('dp', 'tp')), parts along dimension 0
- dy: bfloat16 [3072, 6144], P(('dp', 'tp')), parts along dimension 0
- gate: bfloat16 [3072, 16384], P('dp', 'tp'), parts along dimension 0
- up: bfloat16 [3072, 16384], P('dp', 'tp'), parts along dimension 0
- w_gate: bfloat16 [6144, 16384], P(None, 'tp')
- w_up: bfloat16 [6144, 16384], P(None, 'tp')
- w_down: bfloat16 [16384, 6144], P('tp')
Outputs:
- output 1: bfloat16 [3072, 6144], P(('dp', 'tp')), parts along dimension 0
- output 2: bfloat16 [24576, 16384], P('dp', 'tp'), parts along dimension 0
- output 3: bfloat16 [24576, 16384], P('dp', 'tp'), parts along dimension 0
- output 4: bfloat16 [65536, 6144], P(('dp', 'tp')), parts along dimension 0
There are 4 independent parts. The reference program is written for one: setup_inputs(seed, part) draws one part's arguments, and reference() takes and returns one part's arrays. A program takes and returns all parts, laid end to end along the dimension named above; an argument that names none is the same for every part.
All inputs are finite; a program needn't handle non-finite values.
Results may differ from the reference program's by a relative error of at most 0.012.
Values are sent between devices in bfloat16 or wider.
A program may use at most 1.5 GiB of HBM per device.

```python
import jax
import jax.numpy as jnp

ROWS = 768
D = 6144
FF = 16384


def act(gate, up):
    return jax.nn.silu(gate) * up


def setup_inputs(seed: int = 0, part: int = 0) -> dict:
    kx, ky, ka, kb, kg, ku, kd = jax.random.split(jax.random.key(seed), 7)
    kx, ky, ka, kb = (jax.random.fold_in(k, part) for k in (kx, ky, ka, kb))
    drawn = {
        "x": jax.random.normal(kx, (ROWS, D), jnp.float32),
        "dy": jax.random.normal(ky, (ROWS, D), jnp.float32),
        "gate": jax.random.normal(ka, (ROWS, FF), jnp.float32),
        "up": jax.random.normal(kb, (ROWS, FF), jnp.float32),
        "w_gate": jax.random.normal(kg, (D, FF), jnp.float32) * D**-0.5,
        "w_up": jax.random.normal(ku, (D, FF), jnp.float32) * D**-0.5,
        "w_down": jax.random.normal(kd, (FF, D), jnp.float32) * FF**-0.5,
    }
    return {k: v.astype(jnp.bfloat16) for k, v in drawn.items()}


def reference(x, dy, gate, up, w_gate, w_up, w_down):
    hidden, back = jax.vjp(act, gate.astype(jnp.float32), up.astype(jnp.float32))
    d_hidden = jnp.dot(dy, w_down.T, preferred_element_type=jnp.float32)
    d_gate, d_up = (g.astype(jnp.bfloat16) for g in back(d_hidden))
    dx = jnp.dot(d_gate, w_gate.T, preferred_element_type=jnp.float32) + jnp.dot(d_up, w_up.T, preferred_element_type=jnp.float32)
    dw_gate = jnp.dot(x.T, d_gate, preferred_element_type=jnp.float32)
    dw_up = jnp.dot(x.T, d_up, preferred_element_type=jnp.float32)
    dw_down = jnp.dot(hidden.astype(jnp.bfloat16).T, dy, preferred_element_type=jnp.float32)
    return tuple(g.astype(jnp.bfloat16) for g in (dx, dw_gate, dw_up, dw_down))
```

```python
import functools

import jax
import jax.numpy as jnp
from jax import lax
from jax.experimental import pallas as pl
from jax.experimental.pallas import tpu as pltpu
from jax.sharding import PartitionSpec as P

MESH = pl.DeviceIdType.MESH
BF16, F32 = jnp.bfloat16, jnp.float32
VMEM_LIMIT = 66_000_000

CB = 512
FT = 2048
ET = 512
NT = 256
DT = 384


def dot_nt(a, b):
    return lax.dot_general(a, b, (((1,), (1,)), ((), ())), preferred_element_type=F32)


def dot_tn(a, b):
    return lax.dot_general(a, b, (((0,), (0,)), ((), ())), preferred_element_type=F32)


def ring(n):
    me = lax.axis_index("tp")
    return me, lax.rem(me + 1, n), lax.rem(me + n - 1, n), lax.rem(me + 2, n)


def greet(right, left):
    barrier = pltpu.get_barrier_semaphore()
    for other in (left, right):
        pl.semaphore_signal(barrier, inc=1, device_id={"tp": other}, device_id_type=MESH)
    pl.semaphore_wait(barrier, 2)


def rows_of(device, share, start, size):
    return pl.ds(pl.multiple_of(device * share + start, 16), size)


def remote(src, dst, send, recv, to):
    return pltpu.make_async_remote_copy(
        src_ref=src, dst_ref=dst, send_sem=send, recv_sem=recv, device_id={"tp": to}, device_id_type=MESH
    )


def first_kernel(n, dy, gate, up, wd, dg, du, dwd, dyf, hid_t, acc, wbuf, obuf, gu, eo, lsem, ssem, rsem, wsem, osem, gsem, esem):
    me, right, left, opposite = ring(n)
    share = dy.shape[0]
    half = share // 2
    blocks, _, cb = dyf.shape
    ft = wbuf.shape[1]
    et = gu.shape[-1]
    steps_f = wd.shape[0] // ft
    tiles_e = gate.shape[1] // et
    per_step = ft // et

    def load(j):
        return pltpu.make_async_copy(dy.at[:, pl.ds(pl.multiple_of(j * cb, cb), cb)], dyf.at[j, rows_of(me, share, 0, share), :], lsem.at[j])

    def hop(kind, j, sending):
        to = right if kind % 2 == 0 else left
        if kind < 2:
            start, size = 0, share
            whose = me if sending else (left if kind == 0 else right)
        else:
            start, size = (0 if kind == 2 else half), half
            whose = (left if kind == 2 else right) if sending else opposite
        part = dyf.at[j, rows_of(whose, share, start, size), :]
        return remote(part, part, ssem.at[kind, j], rsem.at[kind, j], to)

    def send_own(j):
        hop(0, j, True).start()
        hop(1, j, True).start()

    def pass_on(j):
        for kind in (0, 1):
            hop(kind, j, False).wait_recv()
        hop(2, j, True).start()
        hop(3, j, True).start()

    def gu_copies(e, slot):
        cols = pl.ds(pl.multiple_of(e * et, et), et)
        return [pltpu.make_async_copy(a.at[:, cols], gu.at[slot, k], gsem.at[slot, k]) for k, a in enumerate((gate, up))]

    def eo_copies(e, slot):
        cols = pl.ds(pl.multiple_of(e * et, et), et)
        return [pltpu.make_async_copy(eo.at[slot, k], a.at[:, cols], esem.at[slot, k]) for k, a in enumerate((dg, du))]

    def tile(ref, j, f):
        return ref.at[pl.ds(pl.multiple_of(f * ft, ft), ft), pl.ds(pl.multiple_of(j * cb, cb), cb)]

    def w_copy(s):
        return pltpu.make_async_copy(tile(wd, s // steps_f, lax.rem(s, steps_f)), wbuf.at[lax.rem(s, 2)], wsem.at[lax.rem(s, 2)])

    def o_copy(s):
        return pltpu.make_async_copy(obuf.at[lax.rem(s, 2)], tile(dwd, s // steps_f, lax.rem(s, steps_f)), osem.at[lax.rem(s, 2)])

    for j in range(blocks):
        load(j).start()
    for c in gu_copies(0, 0):
        c.start()
    w_copy(0).start()
    greet(right, left)
    for j in range(blocks):
        load(j).wait()
        if j < 2:
            send_own(j)

    def hidden_step(e, _):
        slot = lax.rem(e, 2)
        for c in gu_copies(e, slot):
            c.wait()

        @pl.when(e + 1 < tiles_e)
        def _():
            for c in gu_copies(e + 1, 1 - slot):
                c.start()

        g = gu[slot, 0].astype(F32)
        u = gu[slot, 1].astype(F32)
        hidden = (g * jax.nn.sigmoid(g) * u).astype(BF16)
        hid_t[pl.ds(pl.multiple_of(e * et, et), et), :] = hidden.T
        acc[e] = jnp.zeros(acc.shape[1:], F32)
        return 0

    lax.fori_loop(0, tiles_e // 2, hidden_step, 0)
    pass_on(0)
    send_own(2)
    lax.fori_loop(tiles_e // 2, tiles_e, hidden_step, 0)

    total = blocks * steps_f

    def step(s, _):
        j = s // steps_f
        f = lax.rem(s, steps_f)
        slot = lax.rem(s, 2)

        @pl.when(f == 0)
        def _():
            for kind in (2, 3):
                hop(kind, j, False).wait_recv()

            @pl.when(j + 1 < blocks)
            def _():
                pass_on(j + 1)

            @pl.when(j + 3 < blocks)
            def _():
                send_own(j + 3)

        w_copy(s).wait()

        @pl.when(s + 1 < total)
        def _():
            w_copy(s + 1).start()

        @pl.when(s >= 2)
        def _():
            o_copy(s - 2).wait()

        block = dyf[j]
        for q in range(per_step):
            acc[f * per_step + q] += dot_nt(block, wbuf[slot, q * et : (q + 1) * et, :])
        obuf[slot] = jnp.dot(hid_t[pl.ds(pl.multiple_of(f * ft, ft), ft), :], block, preferred_element_type=F32).astype(BF16)
        o_copy(s).start()
        return 0

    for c in gu_copies(0, 0):
        c.start()
    lax.fori_loop(0, total, step, 0)

    def grad_step(e, _):
        slot = lax.rem(e, 2)
        for c in gu_copies(e, slot):
            c.wait()

        @pl.when(e + 1 < tiles_e)
        def _():
            for c in gu_copies(e + 1, 1 - slot):
                c.start()

        @pl.when(e >= 2)
        def _():
            for c in eo_copies(e - 2, slot):
                c.wait()

        g = gu[slot, 0].astype(F32)
        u = gu[slot, 1].astype(F32)
        d = acc[e]
        sig = jax.nn.sigmoid(g)
        silu = g * sig
        eo[slot, 0] = (d * u * (sig + silu * (1.0 - sig))).astype(BF16)
        eo[slot, 1] = (d * silu).astype(BF16)
        for c in eo_copies(e, slot):
            c.start()
        return 0

    lax.fori_loop(0, tiles_e, grad_step, 0)
    for s in (total - 2, total - 1):
        o_copy(s).wait()
    for e in (tiles_e - 2, tiles_e - 1):
        for c in eo_copies(e, e % 2):
            c.wait()
    for j in range(blocks):
        for kind in range(4):
            hop(kind, j, True).wait_send()


def second_kernel(n, dg, du, wg, wu, x, s1r, s1l, s2r, s2l, accr, accl, own, xf, res, lsem, ssem, rsem):
    i = pl.program_id(0)
    steps = pl.num_programs(0)
    me, right, left, opposite = ring(n)
    share = x.shape[0]
    half = share // 2
    quarter = half // 2

    def hop(kind, part, sending):
        to = right if kind % 2 == 0 else left
        if kind < 2:
            whose = me if sending else (left if kind == 0 else right)
        else:
            whose = (left if kind == 2 else right) if sending else opposite
        dst = xf.at[rows_of(whose, share, part * half, half), :]
        src = x.at[pl.ds(part * half, half), :] if sending and kind < 2 else dst
        sem = 2 * kind + part
        return remote(src, dst, ssem.at[sem], rsem.at[sem], to)

    local = pltpu.make_async_copy(x, xf.at[rows_of(me, share, 0, share), :], lsem)

    @pl.when(i == 0)
    def _():
        local.start()
        greet(right, left)
        hop(0, 0, True).start()
        hop(1, 1, True).start()
        hop(0, 1, True).start()
        hop(1, 0, True).start()

    @pl.when(i == steps * 3 // 8)
    def _():
        hop(0, 0, False).wait_recv()
        hop(2, 0, True).start()
        hop(1, 1, False).wait_recv()
        hop(3, 1, True).start()

    res[...] = dot_nt(dg[...], wg[...]) + dot_nt(du[...], wu[...])

    def term(device, start, size):
        return res[rows_of(device, share, start, size), :]

    s1r[:half, :] = term(opposite, 0, half).astype(BF16)
    s1r[half:, :] = term(right, half, quarter).astype(BF16)
    s2r[...] = term(right, half + quarter, quarter).astype(BF16)
    accr[...] = term(right, 0, half)
    s1l[:half, :] = term(opposite, half, half).astype(BF16)
    s1l[half:, :] = term(left, 0, quarter).astype(BF16)
    s2l[...] = term(left, quarter, quarter).astype(BF16)
    accl[...] = term(left, half, half)
    own[...] = term(me, 0, share)

    @pl.when(i == steps - 1)
    def _():
        local.wait()
        hop(0, 1, False).wait_recv()
        hop(1, 0, False).wait_recv()
        hop(2, 0, False).wait_recv()
        hop(3, 1, False).wait_recv()
        for kind, part in ((0, 0), (0, 1), (1, 0), (1, 1), (2, 0), (3, 1)):
            hop(kind, part, True).wait_send()


def gate_kernel(xf, g, out):
    out[...] = dot_tn(xf[...], g[...]).astype(BF16)


def up_kernel(xf, g, ready, out, copied):
    out[...] = dot_tn(xf[...], g[...]).astype(BF16)
    copied[...] = ready[...]


def cost(flops, nbytes):
    return pl.CostEstimate(flops=flops, bytes_accessed=nbytes, transcendentals=0)


def solution(mesh):
    n = mesh.shape["tp"]

    def body(x, dy, gate, up, w_gate, w_up, w_down):
        share, width = x.shape
        rows, ff = gate.shape
        blocks = width // CB
        any_, vmem = pl.BlockSpec(memory_space=pl.ANY), pltpu.VMEM
        flops = 2 * rows * width * ff
        act, wbytes = rows * ff * 2, width * ff * 2
        one = pl.Buffered(1)

        dg, du, dwd = pl.pallas_call(
            functools.partial(first_kernel, n),
            out_shape=[jax.ShapeDtypeStruct((rows, ff), BF16)] * 2 + [jax.ShapeDtypeStruct((ff, width), BF16)],
            in_specs=[any_] * 4,
            out_specs=[any_] * 3,
            scratch_shapes=[
                vmem((blocks, rows, CB), BF16),
                vmem((ff, rows), BF16),
                vmem((ff // ET, rows, ET), F32),
                vmem((2, FT, CB), BF16),
                vmem((2, FT, CB), BF16),
                vmem((2, 2, rows, ET), BF16),
                vmem((2, 2, rows, ET), BF16),
                pltpu.SemaphoreType.DMA((blocks,)),
                pltpu.SemaphoreType.DMA((4, blocks)),
                pltpu.SemaphoreType.DMA((4, blocks)),
                pltpu.SemaphoreType.DMA((2,)),
                pltpu.SemaphoreType.DMA((2,)),
                pltpu.SemaphoreType.DMA((2, 2)),
                pltpu.SemaphoreType.DMA((2, 2)),
            ],
            compiler_params=pltpu.CompilerParams(collective_id=0, has_side_effects=True, vmem_limit_bytes=VMEM_LIMIT),
            cost_estimate=cost(2 * flops, 2 * wbytes + 6 * act),
            name="dhidden_dwdown",
        )(dy, gate, up, w_down)

        half, quarter = share // 2, share // 4

        def strip(count, dtype):
            return jax.ShapeDtypeStruct((count, width), dtype), pl.BlockSpec((count, NT), lambda i: (0, i))

        strips = [strip(half + quarter, BF16)] * 2 + [strip(quarter, BF16)] * 2 + [strip(half, F32)] * 2 + [strip(share, F32)]
        whole = pl.BlockSpec((rows, ff), lambda i: (0, 0), pipeline_mode=one)
        s1r, s1l, s2r, s2l, accr, accl, own, xf = pl.pallas_call(
            functools.partial(second_kernel, n),
            grid=(width // NT,),
            out_shape=[a for a, _ in strips] + [jax.ShapeDtypeStruct((rows, width), BF16)],
            in_specs=[whole, whole, pl.BlockSpec((NT, ff), lambda i: (i, 0)), pl.BlockSpec((NT, ff), lambda i: (i, 0)), any_],
            out_specs=[b for _, b in strips] + [any_],
            scratch_shapes=[
                vmem((rows, NT), F32),
                pltpu.SemaphoreType.DMA,
                pltpu.SemaphoreType.DMA((8,)),
                pltpu.SemaphoreType.DMA((8,)),
            ],
            compiler_params=pltpu.CompilerParams(
                collective_id=1, has_side_effects=True, vmem_limit_bytes=VMEM_LIMIT, dimension_semantics=("arbitrary",)
            ),
            cost_estimate=cost(2 * flops, 2 * wbytes + 6 * act),
            name="dx_gather",
        )(dg, du, w_gate, w_up, x)

        to_right = [(i, (i + 1) % n) for i in range(n)]
        to_left = [(i, (i - 1) % n) for i in range(n)]
        r1r = lax.ppermute(s1r, "tp", to_right)
        r1l = lax.ppermute(s1l, "tp", to_left)

        x_spec = pl.BlockSpec((rows, DT), lambda i: (0, i))
        out_spec = pl.BlockSpec((DT, ff), lambda i: (i, 0))
        plain = pltpu.CompilerParams(vmem_limit_bytes=VMEM_LIMIT, dimension_semantics=("arbitrary",))
        dwg = pl.pallas_call(
            gate_kernel,
            grid=(width // DT,),
            out_shape=jax.ShapeDtypeStruct((width, ff), BF16),
            in_specs=[x_spec, whole],
            out_specs=out_spec,
            compiler_params=plain,
            cost_estimate=cost(flops, wbytes + 3 * act),
            name="dw_gate",
        )(xf, dg)

        s2r = jnp.concatenate([(accr + r1r[:half].astype(F32)).astype(BF16), s2r])
        s2l = jnp.concatenate([(accl + r1l[:half].astype(F32)).astype(BF16), s2l])
        r2r = lax.ppermute(s2r, "tp", to_right)
        r2l = lax.ppermute(s2l, "tp", to_left)

        copy_spec = pl.BlockSpec((ff * DT // width, width), lambda i: (i, 0))
        dwu, dwd = pl.pallas_call(
            up_kernel,
            grid=(width // DT,),
            out_shape=[jax.ShapeDtypeStruct((width, ff), BF16), jax.ShapeDtypeStruct((ff, width), BF16)],
            in_specs=[x_spec, whole, copy_spec],
            out_specs=[out_spec, copy_spec],
            compiler_params=plain,
            cost_estimate=cost(flops, 3 * wbytes + 3 * act),
            name="dw_up",
        )(xf, du, dwd)

        f32 = lambda a: a.astype(F32)
        first = f32(jnp.concatenate([r2r[:half], r2l[:half]]))
        second = f32(jnp.concatenate([r1l[half:], r2l[half:], r1r[half:], r2r[half:]]))
        return (own + first + second).astype(BF16), dwg, dwu, dwd

    part, cols = P(("dp", "tp"), None), P("dp", "tp")
    return jax.shard_map(
        body,
        mesh=mesh,
        in_specs=(part, part, cols, cols, P(None, "tp"), P(None, "tp"), P("tp", None)),
        out_specs=(part, cols, cols, part),
        check_vma=False,
    )
```

```python
import functools

import jax
import jax.numpy as jnp
from jax import lax
from jax.experimental import pallas as pl
from jax.experimental.pallas import tpu as pltpu
from jax.sharding import PartitionSpec as P

MESH = pl.DeviceIdType.MESH
BF16, F32 = jnp.bfloat16, jnp.float32
VMEM_LIMIT = 66_000_000

CB = 512
FT = 1024
ET = 512
NT = 256
DT = 384
XR = 16
DELAY = 4
KEEP = DELAY + 2
SENDS = 4


def dot_nt(a, b):
    return lax.dot_general(a, b, (((1,), (1,)), ((), ())), preferred_element_type=F32)


def dot_tn(a, b):
    return lax.dot_general(a, b, (((0,), (0,)), ((), ())), preferred_element_type=F32)


def ring(n):
    me = lax.axis_index("tp")
    return me, lax.rem(me + 1, n), lax.rem(me + n - 1, n), lax.rem(me + 2, n)


def greet(right, left):
    barrier = pltpu.get_barrier_semaphore()
    for other in (left, right):
        pl.semaphore_signal(barrier, inc=1, device_id={"tp": other}, device_id_type=MESH)
    pl.semaphore_wait(barrier, 2)


def rows_of(device, share, start, size):
    return pl.ds(pl.multiple_of(device * share + start, 16), size)


def remote(src, dst, send, recv, to):
    return pltpu.make_async_remote_copy(
        src_ref=src, dst_ref=dst, send_sem=send, recv_sem=recv, device_id={"tp": to}, device_id_type=MESH
    )


def main_kernel(
    n,
    dy, gate, up, wd, wg, wu, x,
    dg, du, dwd, xf, to_r, to_l, own,
    dyf, hid_t, acc, dgv, duv, wbuf, obuf, gu, w2, rsend, rrecv,
    lsem, ssem, rsem, wsem, osem, gsem, dsem, w2sem, xsend, xrecv, ts, tr, s2sem, owsem,
):
    me, right, left, opposite = ring(n)
    share = dy.shape[0]
    half = share // 2
    blocks, _, cb = dyf.shape
    ft = wbuf.shape[1]
    et = gu.shape[-1]
    steps_f = wd.shape[0] // ft
    tiles_e = gate.shape[1] // et
    per_step = ft // et

    def load(j):
        return pltpu.make_async_copy(dy.at[:, pl.ds(pl.multiple_of(j * cb, cb), cb)], dyf.at[j, rows_of(me, share, 0, share), :], lsem.at[j])

    def hop(kind, j, sending):
        to = right if kind % 2 == 0 else left
        if kind < 2:
            start, size = 0, share
            whose = me if sending else (left if kind == 0 else right)
        else:
            start, size = (0 if kind == 2 else half), half
            whose = (left if kind == 2 else right) if sending else opposite
        part = dyf.at[j, rows_of(whose, share, start, size), :]
        return remote(part, part, ssem.at[kind, j], rsem.at[kind, j], to)

    def send_own(j):
        hop(0, j, True).start()
        hop(1, j, True).start()

    def pass_on(j):
        for kind in (0, 1):
            hop(kind, j, False).wait_recv()
        hop(2, j, True).start()
        hop(3, j, True).start()

    def gu_copies(e, slot):
        cols = pl.ds(pl.multiple_of(e * et, et), et)
        return [pltpu.make_async_copy(a.at[:, cols], gu.at[slot, k], gsem.at[slot, k]) for k, a in enumerate((gate, up))]

    def tile(ref, j, f):
        return ref.at[pl.ds(pl.multiple_of(f * ft, ft), ft), pl.ds(pl.multiple_of(j * cb, cb), cb)]

    def w_copy(s):
        return pltpu.make_async_copy(tile(wd, s // steps_f, lax.rem(s, steps_f)), wbuf.at[lax.rem(s, 2)], wsem.at[lax.rem(s, 2)])

    def o_copy(s):
        return pltpu.make_async_copy(obuf.at[lax.rem(s, 2)], tile(dwd, s // steps_f, lax.rem(s, steps_f)), osem.at[lax.rem(s, 2)])

    chunks = share // XR

    def xhop(kind, c, sending):
        to = right if kind % 2 == 0 else left
        if kind < 2:
            whose = me if sending else (left if kind == 0 else right)
        else:
            whose = (left if kind == 2 else right) if sending else opposite
        dst = xf.at[rows_of(whose, share, c * XR, XR), :]
        src = x.at[pl.ds(pl.multiple_of(c * XR, XR), XR), :] if sending and kind < 2 else dst
        return remote(src, dst, xsend.at[kind, c], xrecv.at[kind, c], to)

    def x_own(k):
        xhop(0, k, True).start()
        xhop(1, lax.rem(k + chunks // 2, chunks), True).start()

    def x_pass(k):
        xhop(0, k, False).wait_recv()
        xhop(2, k, True).start()
        xhop(1, k + chunks // 2, False).wait_recv()
        xhop(3, k + chunks // 2, True).start()

    x_local = pltpu.make_async_copy(x, xf.at[rows_of(me, share, 0, share), :], dsem.at[2])
    x_local.start()
    for j in range(blocks):
        load(j).start()
    for c in gu_copies(0, 0):
        c.start()
    w_copy(0).start()
    greet(right, left)
    for j in range(blocks):
        load(j).wait()
        if j < 2:
            send_own(j)

    def hidden_step(e, _):
        slot = lax.rem(e, 2)
        for c in gu_copies(e, slot):
            c.wait()

        @pl.when(e + 1 < tiles_e)
        def _():
            for c in gu_copies(e + 1, 1 - slot):
                c.start()

        g = gu[slot, 0].astype(F32)
        u = gu[slot, 1].astype(F32)
        hidden = (g * jax.nn.sigmoid(g) * u).astype(BF16)
        hid_t[pl.ds(pl.multiple_of(e * et, et), et), :] = hidden.T
        acc[e] = jnp.zeros(acc.shape[1:], F32)
        return 0

    lax.fori_loop(0, tiles_e // 2, hidden_step, 0)
    pass_on(0)
    send_own(2)
    lax.fori_loop(tiles_e // 2, tiles_e, hidden_step, 0)

    total = blocks * steps_f

    def step(s, _):
        j = s // steps_f
        f = lax.rem(s, steps_f)
        slot = lax.rem(s, 2)

        @pl.when(f == 0)
        def _():
            for kind in (2, 3):
                hop(kind, j, False).wait_recv()

            @pl.when(j + 1 < blocks)
            def _():
                pass_on(j + 1)

            @pl.when(j + 3 < blocks)
            def _():
                send_own(j + 3)

            @pl.when(j + 3 >= blocks)
            def _():
                x_own(j + 3 - blocks)

        w_copy(s).wait()

        @pl.when(s + 1 < total)
        def _():
            w_copy(s + 1).start()

        @pl.when(s >= 2)
        def _():
            o_copy(s - 2).wait()

        block = dyf[j]
        for q in range(per_step):
            acc[f * per_step + q] += dot_nt(block, wbuf[slot, q * et : (q + 1) * et, :])
        obuf[slot] = jnp.dot(hid_t[pl.ds(pl.multiple_of(f * ft, ft), ft), :], block, preferred_element_type=F32).astype(BF16)
        o_copy(s).start()
        return 0

    for c in gu_copies(0, 0):
        c.start()
    lax.fori_loop(0, total, step, 0)

    width = wg.shape[0]
    nt = w2.shape[2]
    tiles = width // nt
    res = acc.at[0, :, :nt]

    def keep(hold, k):
        return acc.at[1 + hold, k * half : (k + 1) * half, :nt]

    def sto(slot):
        return acc.at[1 + KEEP, pl.ds(pl.multiple_of(slot * share, 16), share), :nt]

    def st2(hold, k, start, size):
        return gu.at[hold // 4, k, pl.ds(pl.multiple_of(lax.rem(hold, 4) * share + start, 16), size), :nt]

    def w2_copies(t):
        slot = lax.rem(t, 2)
        part = pl.ds(pl.multiple_of(t * nt, nt), nt)
        return [pltpu.make_async_copy(a.at[part, :], w2.at[slot, k], w2sem.at[slot, k]) for k, a in enumerate((wg, wu))]

    for c in w2_copies(0):
        c.start()
    x_own(3)

    def grad_step(e, _):
        slot = lax.rem(e, 2)
        for c in gu_copies(e, slot):
            c.wait()

        @pl.when(e + 1 < tiles_e)
        def _():
            for c in gu_copies(e + 1, 1 - slot):
                c.start()

        @pl.when(lax.rem(e, 4) == 2)
        def _():
            x_own(4 + e // 4)

        g = gu[slot, 0].astype(F32)
        u = gu[slot, 1].astype(F32)
        d = acc[e]
        sig = jax.nn.sigmoid(g)
        silu = g * sig
        cols = pl.ds(pl.multiple_of(e * et, et), et)
        dgv[:, cols] = (d * u * (sig + silu * (1.0 - sig))).astype(BF16)
        duv[:, cols] = (d * silu).astype(BF16)
        return 0

    lax.fori_loop(0, tiles_e, grad_step, 0)
    d_copies = [pltpu.make_async_copy(v, o, dsem.at[k]) for k, (v, o) in enumerate(((dgv, dg), (duv, du)))]
    for c in d_copies:
        c.start()

    def t_hop(t, k, sending):
        slot = lax.rem(t, SENDS)
        return remote(rsend.at[slot, k], rrecv.at[t, k], ts.at[slot, k], tr.at[t, k], right if k == 0 else left)

    def s2_copies(t):
        slot = lax.rem(t, KEEP)
        part = pl.ds(pl.multiple_of(t * nt, nt), nt)
        return [pltpu.make_async_copy(st2(slot, k, 0, share), a.at[:, part], s2sem.at[slot, k]) for k, a in enumerate((to_r, to_l))]

    def own_copy(t):
        slot = lax.rem(t, 2)
        return pltpu.make_async_copy(sto(slot), own.at[:, pl.ds(pl.multiple_of(t * nt, nt), nt)], owsem.at[slot])

    def dx_step(t, _):
        @pl.when(jnp.logical_and(t >= 1, t <= tiles))
        def _():
            for k in (0, 1):
                t_hop(t - 1, k, True).start()

        @pl.when(jnp.logical_and(lax.rem(t, 4) == 0, t < 2 * chunks))
        def _():
            x_pass(t // 4)

        @pl.when(jnp.logical_and(lax.rem(t, 4) == 2, t < 2 * chunks))
        def _():
            x_own(chunks // 2 + t // 4)

        @pl.when(t < tiles)
        def _():
            slot = lax.rem(t, 2)
            for c in w2_copies(t):
                c.wait()

            @pl.when(t + 1 < tiles)
            def _():
                for c in w2_copies(t + 1):
                    c.start()

            @pl.when(t >= SENDS)
            def _():
                for k in (0, 1):
                    t_hop(t - SENDS, k, True).wait_send()

            @pl.when(t >= KEEP)
            def _():
                for c in s2_copies(t - KEEP):
                    c.wait()

            @pl.when(t >= 2)
            def _():
                own_copy(t - 2).wait()

            res[...] = dot_nt(dgv[...], w2[slot, 0]) + dot_nt(duv[...], w2[slot, 1])

            def term(device, start, size):
                return res[rows_of(device, share, start, size), :]

            hold = lax.rem(t, KEEP)
            out = lax.rem(t, SENDS)
            rsend[out, 0] = term(opposite, 0, half).astype(BF16)
            rsend[out, 1] = term(opposite, half, half).astype(BF16)
            keep(hold, 0)[...] = term(right, 0, half)
            keep(hold, 1)[...] = term(left, half, half)
            st2(hold, 0, half, half)[...] = term(right, half, half).astype(BF16)
            st2(hold, 1, 0, half)[...] = term(left, 0, half).astype(BF16)
            sto(slot)[...] = term(me, 0, share)
            own_copy(t).start()

        @pl.when(t >= DELAY)
        def _():
            u = t - DELAY
            hold = lax.rem(u, KEEP)
            for k in (0, 1):
                t_hop(u, k, False).wait_recv()
            st2(hold, 0, 0, half)[...] = (keep(hold, 0)[...] + rrecv[u, 0].astype(F32)).astype(BF16)
            st2(hold, 1, half, half)[...] = (keep(hold, 1)[...] + rrecv[u, 1].astype(F32)).astype(BF16)
            for c in s2_copies(u):
                c.start()

        return 0

    lax.fori_loop(0, tiles + DELAY, dx_step, 0)

    for s in (total - 2, total - 1):
        o_copy(s).wait()
    for c in d_copies:
        c.wait()
    x_local.wait()
    for t in range(tiles - 2, tiles):
        own_copy(t).wait()
    for t in range(tiles - KEEP, tiles):
        for c in s2_copies(t):
            c.wait()
    for t in range(tiles - SENDS, tiles):
        for k in (0, 1):
            t_hop(t, k, True).wait_send()

    def finish_dy(j, _):
        for kind in range(4):
            hop(kind, j, True).wait_send()
        return 0

    lax.fori_loop(0, blocks, finish_dy, 0)

    def finish_first(c, _):
        xhop(1, c, False).wait_recv()
        xhop(2, c, False).wait_recv()
        xhop(2, c, True).wait_send()
        for kind in (0, 1):
            xhop(kind, c, True).wait_send()
        return 0

    def finish_second(c, _):
        xhop(0, c, False).wait_recv()
        xhop(3, c, False).wait_recv()
        xhop(3, c, True).wait_send()
        for kind in (0, 1):
            xhop(kind, c, True).wait_send()
        return 0

    lax.fori_loop(0, chunks // 2, finish_first, 0)
    lax.fori_loop(chunks // 2, chunks, finish_second, 0)


def dw_kernel(xf, dg, du, ready, dwg, dwu, copied):
    t = xf[...]
    dwg[...] = dot_tn(t, dg[...]).astype(BF16)
    dwu[...] = dot_tn(t, du[...]).astype(BF16)
    copied[...] = ready[...]


def cost(flops, nbytes):
    return pl.CostEstimate(flops=flops, bytes_accessed=nbytes, transcendentals=0)


def solution(mesh):
    n = mesh.shape["tp"]

    def body(x, dy, gate, up, w_gate, w_up, w_down):
        share, width = x.shape
        rows, ff = gate.shape
        blocks, tiles, half = width // CB, width // NT, share // 2
        any_, vmem, dma = pl.BlockSpec(memory_space=pl.ANY), pltpu.VMEM, pltpu.SemaphoreType.DMA
        flops = 2 * rows * width * ff
        act, wbytes = rows * ff * 2, width * ff * 2
        shape = jax.ShapeDtypeStruct

        dg, du, dwd, xf, to_r, to_l, own = pl.pallas_call(
            functools.partial(main_kernel, n),
            out_shape=[
                shape((rows, ff), BF16),
                shape((rows, ff), BF16),
                shape((ff, width), BF16),
                shape((rows, width), BF16),
                shape((share, width), BF16),
                shape((share, width), BF16),
                shape((share, width), F32),
            ],
            in_specs=[any_] * 7,
            out_specs=[any_] * 7,
            scratch_shapes=[
                vmem((blocks, rows, CB), BF16),
                vmem((ff, rows), BF16),
                vmem((ff // ET, rows, ET), F32),
                vmem((rows, ff), BF16),
                vmem((rows, ff), BF16),
                vmem((2, FT, CB), BF16),
                vmem((2, FT, CB), BF16),
                vmem((2, 2, rows, ET), BF16),
                vmem((2, 2, NT, ff), BF16),
                vmem((SENDS, 2, half, NT), BF16),
                vmem((tiles, 2, half, NT), BF16),
                dma((blocks,)),
                dma((4, blocks)),
                dma((4, blocks)),
                dma((2,)),
                dma((2,)),
                dma((2, 2)),
                dma((3,)),
                dma((2, 2)),
                dma((4, share // XR)),
                dma((4, share // XR)),
                dma((SENDS, 2)),
                dma((tiles, 2)),
                dma((KEEP, 2)),
                dma((2,)),
            ],
            compiler_params=pltpu.CompilerParams(collective_id=0, has_side_effects=True, vmem_limit_bytes=VMEM_LIMIT),
            cost_estimate=cost(4 * flops, 4 * wbytes + 8 * act),
            name="dhidden_dwdown_dx",
        )(dy, gate, up, w_down, w_gate, w_up, x)

        from_l = lax.ppermute(to_r, "tp", [(i, (i + 1) % n) for i in range(n)])
        from_r = lax.ppermute(to_l, "tp", [(i, (i - 1) % n) for i in range(n)])

        whole = pl.BlockSpec((rows, ff), lambda i: (0, 0), pipeline_mode=pl.Buffered(1))
        out_spec = pl.BlockSpec((DT, ff), lambda i: (i, 0))
        copy_spec = pl.BlockSpec((ff * DT // width, width), lambda i: (i, 0))
        dwg, dwu, dwd = pl.pallas_call(
            dw_kernel,
            grid=(width // DT,),
            out_shape=[shape((width, ff), BF16), shape((width, ff), BF16), shape((ff, width), BF16)],
            in_specs=[pl.BlockSpec((rows, DT), lambda i: (0, i)), whole, whole, copy_spec],
            out_specs=[out_spec, out_spec, copy_spec],
            compiler_params=pltpu.CompilerParams(vmem_limit_bytes=VMEM_LIMIT, dimension_semantics=("arbitrary",)),
            cost_estimate=cost(2 * flops, 4 * wbytes + 4 * act),
            name="dw_gate_up",
        )(xf, dg, du, dwd)

        dx = (own + from_l.astype(F32) + from_r.astype(F32)).astype(BF16)
        return dx, dwg, dwu, dwd

    part, cols = P(("dp", "tp"), None), P("dp", "tp")
    return jax.shard_map(
        body,
        mesh=mesh,
        in_specs=(part, part, cols, cols, P(None, "tp"), P(None, "tp"), P("tp", None)),
        out_specs=(part, cols, cols, part),
        check_vma=False,
    )
```

```python
import functools

import jax
import jax.numpy as jnp
from jax import lax
from jax.experimental import pallas as pl
from jax.experimental.pallas import tpu as pltpu
from jax.sharding import PartitionSpec as P

MESH = pl.DeviceIdType.MESH
BF16, F32 = jnp.bfloat16, jnp.float32
VMEM_LIMIT = 66_000_000

CB = 512
FT = 2048
ET = 512
NT = 256
DT = 384
XR = 16
DELAY = 5
KEEP = DELAY + 1
SENDS = 4


def dot_nt(a, b):
    return lax.dot_general(a, b, (((1,), (1,)), ((), ())), preferred_element_type=F32)


def dot_tn(a, b):
    return lax.dot_general(a, b, (((0,), (0,)), ((), ())), preferred_element_type=F32)


def ring(n):
    me = lax.axis_index("tp")
    return me, lax.rem(me + 1, n), lax.rem(me + n - 1, n), lax.rem(me + 2, n)


def greet(right, left):
    barrier = pltpu.get_barrier_semaphore()
    for other in (left, right):
        pl.semaphore_signal(barrier, inc=1, device_id={"tp": other}, device_id_type=MESH)
    pl.semaphore_wait(barrier, 2)


def rows_of(device, share, start, size):
    return pl.ds(pl.multiple_of(device * share + start, 16), size)


def remote(src, dst, send, recv, to):
    return pltpu.make_async_remote_copy(
        src_ref=src, dst_ref=dst, send_sem=send, recv_sem=recv, device_id={"tp": to}, device_id_type=MESH
    )


def main_kernel(
    n,
    dy, gate, up, wd, wg, wu, x,
    dg, du, dwd, xf, to_r, to_l, own,
    dyf, hid_t, acc, dgv, duv, wbuf, gu, w2, rsend, rrecv,
    lsem, ssem, rsem, wsem, osem, gsem, dsem, w2sem, xsend, xrecv, ts, tr, s2sem, owsem,
):
    me, right, left, opposite = ring(n)
    share = dy.shape[0]
    half = share // 2
    blocks, _, cb = dyf.shape
    ft = wbuf.shape[1]
    et = gu.shape[-1]
    steps_f = wd.shape[0] // ft
    tiles_e = gate.shape[1] // et
    per_step = ft // et

    def load(j):
        return pltpu.make_async_copy(dy.at[:, pl.ds(pl.multiple_of(j * cb, cb), cb)], dyf.at[j, rows_of(me, share, 0, share), :], lsem.at[j])

    def hop(kind, j, sending):
        to = right if kind % 2 == 0 else left
        if kind < 4:
            whose = me if sending else (left if kind % 2 == 0 else right)
        else:
            whose = (left if kind == 4 else right) if sending else opposite
        part = dyf.at[j, rows_of(whose, share, half if kind in (1, 2, 5) else 0, half), :]
        return remote(part, part, ssem.at[kind, j], rsem.at[kind, j], to)

    def send_own(j):
        for kind in range(4):
            hop(kind, j, True).start()

    def pass_on(j):
        for kind in (0, 1):
            hop(kind, j, False).wait_recv()
            hop(kind + 4, j, True).start()

    def gu_copies(e, slot):
        cols = pl.ds(pl.multiple_of(e * et, et), et)
        return [pltpu.make_async_copy(a.at[:, cols], gu.at[slot, k], gsem.at[slot, k]) for k, a in enumerate((gate, up))]

    def tile(ref, j, f):
        return ref.at[pl.ds(pl.multiple_of(f * ft, ft), ft), pl.ds(pl.multiple_of(j * cb, cb), cb)]

    def w_copy(s):
        return pltpu.make_async_copy(tile(wd, s // steps_f, lax.rem(s, steps_f)), wbuf.at[lax.rem(s, 2)], wsem.at[lax.rem(s, 2)])

    nt = w2.shape[2]
    panels = ft // nt

    def panel(slot, q):
        return w2.at[1, slot, :, q * cb : (q + 1) * cb]

    def o_copies(s):
        slot = lax.rem(s, 2)
        cols = pl.ds(pl.multiple_of(s // steps_f * cb, cb), cb)
        start = lax.rem(s, steps_f) * ft
        return [
            pltpu.make_async_copy(panel(slot, q), dwd.at[pl.ds(pl.multiple_of(start + q * nt, nt), nt), cols], osem.at[slot, q])
            for q in range(panels)
        ]

    chunks = share // XR

    def xhop(kind, c, sending):
        to = right if kind % 2 == 0 else left
        if kind < 2:
            whose = me if sending else (left if kind == 0 else right)
        else:
            whose = (left if kind == 2 else right) if sending else opposite
        dst = xf.at[rows_of(whose, share, c * XR, XR), :]
        src = x.at[pl.ds(pl.multiple_of(c * XR, XR), XR), :] if sending and kind < 2 else dst
        return remote(src, dst, xsend.at[kind, c], xrecv.at[kind, c], to)

    def x_own(k):
        xhop(0, k, True).start()
        xhop(1, lax.rem(k + chunks // 2, chunks), True).start()

    def x_pass(k):
        xhop(0, k, False).wait_recv()
        xhop(2, k, True).start()
        xhop(1, k + chunks // 2, False).wait_recv()
        xhop(3, k + chunks // 2, True).start()

    x_local = pltpu.make_async_copy(x, xf.at[rows_of(me, share, 0, share), :], dsem.at[2])
    x_local.start()
    for j in range(blocks):
        load(j).start()
    for c in gu_copies(0, 0):
        c.start()
    w_copy(0).start()
    greet(right, left)
    for j in range(blocks):
        load(j).wait()
        if j == 0:
            send_own(0)

    def hidden_step(e, _):
        slot = lax.rem(e, 2)
        for c in gu_copies(e, slot):
            c.wait()

        @pl.when(e + 1 < tiles_e)
        def _():
            for c in gu_copies(e + 1, 1 - slot):
                c.start()

        g = gu[slot, 0].astype(F32)
        u = gu[slot, 1].astype(F32)
        hidden = (g * jax.nn.sigmoid(g) * u).astype(BF16)
        hid_t[pl.ds(pl.multiple_of(e * et, et), et), :] = hidden.T
        acc[e] = jnp.zeros(acc.shape[1:], F32)
        return 0

    lax.fori_loop(0, tiles_e * 3 // 8, hidden_step, 0)
    pass_on(0)
    send_own(1)
    send_own(2)
    lax.fori_loop(tiles_e * 3 // 8, tiles_e, hidden_step, 0)

    total = blocks * steps_f

    def step(s, _):
        j = s // steps_f
        f = lax.rem(s, steps_f)
        slot = lax.rem(s, 2)

        @pl.when(f == 0)
        def _():
            for kind in (2, 3, 4, 5):
                hop(kind, j, False).wait_recv()

            @pl.when(j + 1 < blocks)
            def _():
                pass_on(j + 1)

            @pl.when(j + 3 < blocks)
            def _():
                send_own(j + 3)

            @pl.when(j + 3 >= blocks)
            def _():
                x_own(j + 3 - blocks)

        w_copy(s).wait()

        @pl.when(s + 1 < total)
        def _():
            w_copy(s + 1).start()

        @pl.when(s >= 2)
        def _():
            for c in o_copies(s - 2):
                c.wait()

        block = dyf[j]
        for q in range(per_step):
            acc[f * per_step + q] += dot_nt(block, wbuf[slot, q * et : (q + 1) * et, :])
        product = jnp.dot(hid_t[pl.ds(pl.multiple_of(f * ft, ft), ft), :], block, preferred_element_type=F32).astype(BF16)
        for q in range(panels):
            panel(slot, q)[...] = product[q * nt : (q + 1) * nt]
        for c in o_copies(s):
            c.start()
        return 0

    for c in gu_copies(0, 0):
        c.start()
    lax.fori_loop(0, total, step, 0)

    width = wg.shape[0]
    tiles = width // nt
    def res(slot):
        return acc.at[slot, :, :nt]

    def keep(hold, k):
        return acc.at[2 + hold, k * half : (k + 1) * half, :nt]

    def sto(slot):
        return acc.at[0, pl.ds(pl.multiple_of(slot * share, 16), share), nt : 2 * nt]

    def st2(hold, k, start, size):
        return gu.at[hold // 4, k, pl.ds(pl.multiple_of(lax.rem(hold, 4) * share + start, 16), size), :nt]

    def w2_copies(t):
        slot = lax.rem(t, 2)
        part = pl.ds(pl.multiple_of(t * nt, nt), nt)
        return [pltpu.make_async_copy(a.at[part, :], w2.at[slot, k], w2sem.at[slot, k]) for k, a in enumerate((wg, wu))]

    for c in w2_copies(0):
        c.start()
    x_own(3)

    def grad_step(e, _):
        slot = lax.rem(e, 2)
        for c in gu_copies(e, slot):
            c.wait()

        @pl.when(e + 1 < tiles_e)
        def _():
            for c in gu_copies(e + 1, 1 - slot):
                c.start()

        @pl.when(lax.rem(e, 4) == 2)
        def _():
            x_own(4 + e // 4)

        g = gu[slot, 0].astype(F32)
        u = gu[slot, 1].astype(F32)
        d = acc[e]
        sig = jax.nn.sigmoid(g)
        silu = g * sig
        cols = pl.ds(pl.multiple_of(e * et, et), et)
        dgv[:, cols] = (d * u * (sig + silu * (1.0 - sig))).astype(BF16)
        duv[:, cols] = (d * silu).astype(BF16)
        return 0

    lax.fori_loop(0, tiles_e, grad_step, 0)
    d_copies = [pltpu.make_async_copy(v, o, dsem.at[k]) for k, (v, o) in enumerate(((dgv, dg), (duv, du)))]
    for c in d_copies:
        c.start()

    def t_hop(t, k, sending):
        slot = lax.rem(t, SENDS)
        return remote(rsend.at[slot, k], rrecv.at[t, k], ts.at[slot, k], tr.at[t, k], right if k == 0 else left)

    def s2_copies(t):
        slot = lax.rem(t, KEEP)
        part = pl.ds(pl.multiple_of(t * nt, nt), nt)
        return [pltpu.make_async_copy(st2(slot, k, 0, share), a.at[:, part], s2sem.at[slot, k]) for k, a in enumerate((to_r, to_l))]

    def own_copy(t):
        slot = lax.rem(t, 2)
        return pltpu.make_async_copy(sto(slot), own.at[:, pl.ds(pl.multiple_of(t * nt, nt), nt)], owsem.at[slot])

    def free_slots(p):
        @pl.when(p >= SENDS)
        def _():
            for k in (0, 1):
                t_hop(p - SENDS, k, True).wait_send()

        @pl.when(p >= KEEP)
        def _():
            for c in s2_copies(p - KEEP):
                c.wait()

        @pl.when(p >= 2)
        def _():
            own_copy(p - 2).wait()

    def strips(slot, hold, out):
        def term(device, start, size):
            return res(slot)[rows_of(device, share, start, size), :]

        rsend[out, 0] = term(opposite, 0, half).astype(BF16)
        rsend[out, 1] = term(opposite, half, half).astype(BF16)
        keep(hold, 0)[...] = term(right, 0, half)
        keep(hold, 1)[...] = term(left, half, half)
        st2(hold, 0, half, half)[...] = term(right, half, half).astype(BF16)
        st2(hold, 1, 0, half)[...] = term(left, 0, half).astype(BF16)
        sto(slot)[...] = term(me, 0, share)

    def arrive(u):
        hold = lax.rem(u, KEEP)
        for k in (0, 1):
            t_hop(u, k, False).wait_recv()
        st2(hold, 0, 0, half)[...] = (keep(hold, 0)[...] + rrecv[u, 0].astype(F32)).astype(BF16)
        st2(hold, 1, half, half)[...] = (keep(hold, 1)[...] + rrecv[u, 1].astype(F32)).astype(BF16)
        for c in s2_copies(u):
            c.start()

    for s in (total - 2, total - 1):
        for c in o_copies(s):
            c.wait()

    def dx_step(t, _):
        @pl.when(t >= 2)
        def _():
            for k in (0, 1):
                t_hop(t - 2, k, True).start()

        @pl.when(jnp.logical_and(lax.rem(t, 4) == 0, t < 2 * chunks))
        def _():
            x_pass(t // 4)

        @pl.when(jnp.logical_and(lax.rem(t, 4) == 2, t < 2 * chunks))
        def _():
            x_own(chunks // 2 + t // 4)

        @pl.when(t >= DELAY)
        def _():
            arrive(t - DELAY)

        slot = lax.rem(t, 2)
        for c in w2_copies(t):
            c.wait()

        @pl.when(t + 1 < tiles)
        def _():
            for c in w2_copies(t + 1):
                c.start()

        free_slots(t - 1)
        res(slot)[...] = dot_nt(dgv[...], w2[slot, 0]) + dot_nt(duv[...], w2[slot, 1])
        strips(1 - slot, lax.rem(t + KEEP - 1, KEEP), lax.rem(t + SENDS - 1, SENDS))

        @pl.when(t >= 1)
        def _():
            own_copy(t - 1).start()

        return 0

    lax.fori_loop(0, tiles, dx_step, 0)
    last = tiles - 1
    for k in (0, 1):
        t_hop(last - 1, k, True).start()
    free_slots(last)
    strips(last % 2, last % KEEP, last % SENDS)
    own_copy(last).start()
    for k in (0, 1):
        t_hop(last, k, True).start()

    def late(u, _):
        arrive(u)
        return 0

    lax.fori_loop(tiles - DELAY, tiles, late, 0)
    for c in d_copies:
        c.wait()
    x_local.wait()
    for t in range(tiles - 2, tiles):
        own_copy(t).wait()
    for t in range(tiles - KEEP, tiles):
        for c in s2_copies(t):
            c.wait()
    for t in range(tiles - SENDS, tiles):
        for k in (0, 1):
            t_hop(t, k, True).wait_send()

    def finish_dy(j, _):
        for kind in range(6):
            hop(kind, j, True).wait_send()
        return 0

    lax.fori_loop(0, blocks, finish_dy, 0)

    def finish_first(c, _):
        xhop(1, c, False).wait_recv()
        xhop(2, c, False).wait_recv()
        xhop(2, c, True).wait_send()
        for kind in (0, 1):
            xhop(kind, c, True).wait_send()
        return 0

    def finish_second(c, _):
        xhop(0, c, False).wait_recv()
        xhop(3, c, False).wait_recv()
        xhop(3, c, True).wait_send()
        for kind in (0, 1):
            xhop(kind, c, True).wait_send()
        return 0

    lax.fori_loop(0, chunks // 2, finish_first, 0)
    lax.fori_loop(chunks // 2, chunks, finish_second, 0)


def dw_kernel(xf, dg, du, ready, dwg, dwu, copied, cbuf, isem, osem):
    i = pl.program_id(0)
    steps = pl.num_programs(0)
    size = cbuf.shape[1]

    def copies(c):
        slot = lax.rem(c, 2)
        part = pl.ds(pl.multiple_of(c * size, size), size)
        return (
            pltpu.make_async_copy(ready.at[part, :], cbuf.at[slot], isem.at[slot]),
            pltpu.make_async_copy(cbuf.at[slot], copied.at[part, :], osem.at[slot]),
        )

    @pl.when(lax.rem(i, 2) == 0)
    def _():
        @pl.when(i >= 4)
        def _():
            copies(i // 2 - 2)[1].wait()

        copies(i // 2)[0].start()

    @pl.when(lax.rem(i, 2) == 1)
    def _():
        copies(i // 2)[0].wait()
        copies(i // 2)[1].start()

    t = xf[...]
    dwg[...] = dot_tn(t, dg[...]).astype(BF16)
    dwu[...] = dot_tn(t, du[...]).astype(BF16)

    @pl.when(i == steps - 1)
    def _():
        copies(steps // 2 - 2)[1].wait()
        copies(steps // 2 - 1)[1].wait()


def cost(flops, nbytes):
    return pl.CostEstimate(flops=flops, bytes_accessed=nbytes, transcendentals=0)


def solution(mesh):
    n = mesh.shape["tp"]

    def body(x, dy, gate, up, w_gate, w_up, w_down):
        share, width = x.shape
        rows, ff = gate.shape
        blocks, tiles, half = width // CB, width // NT, share // 2
        any_, vmem, dma = pl.BlockSpec(memory_space=pl.ANY), pltpu.VMEM, pltpu.SemaphoreType.DMA
        flops = 2 * rows * width * ff
        act, wbytes = rows * ff * 2, width * ff * 2
        shape = jax.ShapeDtypeStruct

        dg, du, dwd, xf, to_r, to_l, own = pl.pallas_call(
            functools.partial(main_kernel, n),
            out_shape=[
                shape((rows, ff), BF16),
                shape((rows, ff), BF16),
                shape((ff, width), BF16),
                shape((rows, width), BF16),
                shape((share, width), BF16),
                shape((share, width), BF16),
                shape((share, width), F32),
            ],
            in_specs=[any_] * 7,
            out_specs=[any_] * 7,
            scratch_shapes=[
                vmem((blocks, rows, CB), BF16),
                vmem((ff, rows), BF16),
                vmem((ff // ET, rows, ET), F32),
                vmem((rows, ff), BF16),
                vmem((rows, ff), BF16),
                vmem((2, FT, CB), BF16),
                vmem((2, 2, rows, ET), BF16),
                vmem((2, 2, NT, ff), BF16),
                vmem((SENDS, 2, half, NT), BF16),
                vmem((tiles, 2, half, NT), BF16),
                dma((blocks,)),
                dma((6, blocks)),
                dma((6, blocks)),
                dma((2,)),
                dma((2, FT // NT)),
                dma((2, 2)),
                dma((3,)),
                dma((2, 2)),
                dma((4, share // XR)),
                dma((4, share // XR)),
                dma((SENDS, 2)),
                dma((tiles, 2)),
                dma((KEEP, 2)),
                dma((2,)),
            ],
            compiler_params=pltpu.CompilerParams(collective_id=0, has_side_effects=True, vmem_limit_bytes=VMEM_LIMIT),
            cost_estimate=cost(4 * flops, 4 * wbytes + 8 * act),
            name="dhidden_dwdown_dx",
        )(dy, gate, up, w_down, w_gate, w_up, x)

        from_l = lax.ppermute(to_r, "tp", [(i, (i + 1) % n) for i in range(n)])
        from_r = lax.ppermute(to_l, "tp", [(i, (i - 1) % n) for i in range(n)])

        whole = pl.BlockSpec((rows, ff), lambda i: (0, 0), pipeline_mode=pl.Buffered(1))
        out_spec = pl.BlockSpec((DT, ff), lambda i: (i, 0))
        dwg, dwu, dwd = pl.pallas_call(
            dw_kernel,
            grid=(width // DT,),
            out_shape=[shape((width, ff), BF16), shape((width, ff), BF16), shape((ff, width), BF16)],
            in_specs=[pl.BlockSpec((rows, DT), lambda i: (0, i)), whole, whole, any_],
            out_specs=[out_spec, out_spec, any_],
            scratch_shapes=[vmem((2, ff * DT * 2 // width, width), BF16), dma((2,)), dma((2,))],
            compiler_params=pltpu.CompilerParams(vmem_limit_bytes=50_000_000, dimension_semantics=("arbitrary",)),
            cost_estimate=cost(2 * flops, 4 * wbytes + 4 * act),
            name="dw_gate_up",
        )(xf, dg, du, dwd)

        dx = (own + from_l.astype(F32) + from_r.astype(F32)).astype(BF16)
        return dx, dwg, dwu, dwd

    part, cols = P(("dp", "tp"), None), P("dp", "tp")
    return jax.shard_map(
        body,
        mesh=mesh,
        in_specs=(part, part, cols, cols, P(None, "tp"), P(None, "tp"), P("tp", None)),
        out_specs=(part, cols, cols, part),
        check_vma=False,
    )
```

```python
import functools

import jax
import jax.numpy as jnp
from jax import lax
from jax.experimental import pallas as pl
from jax.experimental.pallas import tpu as pltpu
from jax.sharding import PartitionSpec as P

MESH = pl.DeviceIdType.MESH
BF16, F32 = jnp.bfloat16, jnp.float32
VMEM_LIMIT = 66_000_000

CB = 512
FT = 2048
ET = 512
NT = 256
DT = 384
XR = 16
DELAY = 5
KEEP = DELAY + 1
SENDS = 4


def dot_nt(a, b):
    return lax.dot_general(a, b, (((1,), (1,)), ((), ())), preferred_element_type=F32)


def dot_tn(a, b):
    return lax.dot_general(a, b, (((0,), (0,)), ((), ())), preferred_element_type=F32)


def ring(n):
    me = lax.axis_index("tp")
    return me, lax.rem(me + 1, n), lax.rem(me + n - 1, n), lax.rem(me + 2, n)


def greet(right, left):
    barrier = pltpu.get_barrier_semaphore()
    for other in (left, right):
        pl.semaphore_signal(barrier, inc=1, device_id={"tp": other}, device_id_type=MESH)
    pl.semaphore_wait(barrier, 2)


def rows_of(device, share, start, size):
    return pl.ds(pl.multiple_of(device * share + start, 16), size)


def remote(src, dst, send, recv, to):
    return pltpu.make_async_remote_copy(
        src_ref=src, dst_ref=dst, send_sem=send, recv_sem=recv, device_id={"tp": to}, device_id_type=MESH
    )


def main_kernel(
    n,
    dy, gate, up, wd, wg, wu, x,
    dg, du, dwd, xf, to_r, to_l, own,
    dyf, hid_t, acc, dgv, duv, wbuf, gu, w2, rsend, rrecv,
    lsem, ssem, rsem, wsem, osem, gsem, dsem, w2sem, xsend, xrecv, ts, tr, s2sem, owsem,
):
    me, right, left, opposite = ring(n)
    share = dy.shape[0]
    half = share // 2
    blocks, _, cb = dyf.shape
    ft = wbuf.shape[1]
    et = gu.shape[-1]
    steps_f = wd.shape[0] // ft
    tiles_e = gate.shape[1] // et
    per_step = ft // et

    def load(j):
        return pltpu.make_async_copy(dy.at[:, pl.ds(pl.multiple_of(j * cb, cb), cb)], dyf.at[j, rows_of(me, share, 0, share), :], lsem.at[j])

    def hop(kind, j, sending):
        to = right if kind % 2 == 0 else left
        if kind < 4:
            whose = me if sending else (left if kind % 2 == 0 else right)
        else:
            whose = (left if kind == 4 else right) if sending else opposite
        part = dyf.at[j, rows_of(whose, share, half if kind in (1, 2, 5) else 0, half), :]
        return remote(part, part, ssem.at[kind, j], rsem.at[kind, j], to)

    def send_own(j):
        for kind in range(4):
            hop(kind, j, True).start()

    def pass_on(j):
        for kind in (0, 1):
            hop(kind, j, False).wait_recv()
            hop(kind + 4, j, True).start()

    def gu_copies(e, slot):
        cols = pl.ds(pl.multiple_of(e * et, et), et)
        return [pltpu.make_async_copy(a.at[:, cols], gu.at[slot, k], gsem.at[slot, k]) for k, a in enumerate((gate, up))]

    def tile(ref, j, f):
        return ref.at[pl.ds(pl.multiple_of(f * ft, ft), ft), pl.ds(pl.multiple_of(j * cb, cb), cb)]

    def w_copy(s):
        return pltpu.make_async_copy(tile(wd, s // steps_f, lax.rem(s, steps_f)), wbuf.at[lax.rem(s, 2)], wsem.at[lax.rem(s, 2)])

    nt = w2.shape[2]
    panels = ft // nt

    def panel(slot, q):
        return w2.at[1, slot, :, q * cb : (q + 1) * cb]

    def o_copies(s):
        slot = lax.rem(s, 2)
        cols = pl.ds(pl.multiple_of(s // steps_f * cb, cb), cb)
        start = lax.rem(s, steps_f) * ft
        return [
            pltpu.make_async_copy(panel(slot, q), dwd.at[pl.ds(pl.multiple_of(start + q * nt, nt), nt), cols], osem.at[slot, q])
            for q in range(panels)
        ]

    chunks = share // XR

    def xhop(kind, c, sending):
        to = right if kind % 2 == 0 else left
        if kind < 2:
            whose = me if sending else (left if kind == 0 else right)
        else:
            whose = (left if kind == 2 else right) if sending else opposite
        dst = xf.at[rows_of(whose, share, c * XR, XR), :]
        src = x.at[pl.ds(pl.multiple_of(c * XR, XR), XR), :] if sending and kind < 2 else dst
        return remote(src, dst, xsend.at[kind, c], xrecv.at[kind, c], to)

    def x_own(k):
        xhop(0, k, True).start()
        xhop(1, lax.rem(k + chunks // 2, chunks), True).start()

    def x_pass(k):
        xhop(0, k, False).wait_recv()
        xhop(2, k, True).start()
        xhop(1, k + chunks // 2, False).wait_recv()
        xhop(3, k + chunks // 2, True).start()

    x_local = pltpu.make_async_copy(x, xf.at[rows_of(me, share, 0, share), :], dsem.at[2])
    x_local.start()
    for j in range(blocks):
        load(j).start()
    for c in gu_copies(0, 0):
        c.start()
    w_copy(0).start()
    greet(right, left)
    for j in range(blocks):
        load(j).wait()
        if j == 0:
            send_own(0)

    def hidden_step(e, _):
        slot = lax.rem(e, 2)
        for c in gu_copies(e, slot):
            c.wait()

        @pl.when(e + 1 < tiles_e)
        def _():
            for c in gu_copies(e + 1, 1 - slot):
                c.start()

        g = gu[slot, 0].astype(F32)
        u = gu[slot, 1].astype(F32)
        hidden = (g * jax.nn.sigmoid(g) * u).astype(BF16)
        hid_t[pl.ds(pl.multiple_of(e * et, et), et), :] = hidden.T
        acc[e] = jnp.zeros(acc.shape[1:], F32)
        return 0

    lax.fori_loop(0, tiles_e * 3 // 8, hidden_step, 0)
    pass_on(0)
    send_own(1)
    send_own(2)
    lax.fori_loop(tiles_e * 3 // 8, tiles_e, hidden_step, 0)

    total = blocks * steps_f

    def step(s, _):
        j = s // steps_f
        f = lax.rem(s, steps_f)
        slot = lax.rem(s, 2)

        @pl.when(f == 0)
        def _():
            for kind in (2, 3, 4, 5):
                hop(kind, j, False).wait_recv()

            @pl.when(j + 1 < blocks)
            def _():
                pass_on(j + 1)

            @pl.when(j + 3 < blocks)
            def _():
                send_own(j + 3)

            @pl.when(j + 3 >= blocks)
            def _():
                x_own(j + 3 - blocks)

        w_copy(s).wait()

        @pl.when(s + 1 < total)
        def _():
            w_copy(s + 1).start()

        @pl.when(s >= 2)
        def _():
            for c in o_copies(s - 2):
                c.wait()

        block = dyf[j]
        for q in range(per_step):
            acc[f * per_step + q] += dot_nt(block, wbuf[slot, q * et : (q + 1) * et, :])
        product = jnp.dot(hid_t[pl.ds(pl.multiple_of(f * ft, ft), ft), :], block, preferred_element_type=F32).astype(BF16)
        for q in range(panels):
            panel(slot, q)[...] = product[q * nt : (q + 1) * nt]
        for c in o_copies(s):
            c.start()
        return 0

    for c in gu_copies(0, 0):
        c.start()
    lax.fori_loop(0, total, step, 0)

    width = wg.shape[0]
    tiles = width // nt
    def res(slot):
        return acc.at[slot, :, :nt]

    def keep(hold, k):
        return acc.at[2 + hold, k * half : (k + 1) * half, :nt]

    def sto(slot):
        return acc.at[0, pl.ds(pl.multiple_of(slot * share, 16), share), nt : 2 * nt]

    def st2(hold, k, start, size):
        return gu.at[hold // 4, k, pl.ds(pl.multiple_of(lax.rem(hold, 4) * share + start, 16), size), :nt]

    def w2_copies(t):
        slot = lax.rem(t, 2)
        part = pl.ds(pl.multiple_of(t * nt, nt), nt)
        return [pltpu.make_async_copy(a.at[part, :], w2.at[slot, k], w2sem.at[slot, k]) for k, a in enumerate((wg, wu))]

    for c in w2_copies(0):
        c.start()
    x_own(3)

    def grad_step(e, _):
        slot = lax.rem(e, 2)
        for c in gu_copies(e, slot):
            c.wait()

        @pl.when(e + 1 < tiles_e)
        def _():
            for c in gu_copies(e + 1, 1 - slot):
                c.start()

        @pl.when(lax.rem(e, 4) == 2)
        def _():
            x_own(4 + e // 4)

        g = gu[slot, 0].astype(F32)
        u = gu[slot, 1].astype(F32)
        d = acc[e]
        sig = jax.nn.sigmoid(g)
        silu = g * sig
        cols = pl.ds(pl.multiple_of(e * et, et), et)
        dgv[:, cols] = (d * u * (sig + silu * (1.0 - sig))).astype(BF16)
        duv[:, cols] = (d * silu).astype(BF16)
        return 0

    lax.fori_loop(0, tiles_e, grad_step, 0)
    d_copies = [pltpu.make_async_copy(v, o, dsem.at[k]) for k, (v, o) in enumerate(((dgv, dg), (duv, du)))]
    for c in d_copies:
        c.start()

    def t_hop(t, k, sending):
        slot = lax.rem(t, SENDS)
        return remote(rsend.at[slot, k], rrecv.at[t, k], ts.at[slot, k], tr.at[t, k], right if k == 0 else left)

    def s2_copies(t):
        slot = lax.rem(t, KEEP)
        part = pl.ds(pl.multiple_of(t * nt, nt), nt)
        return [pltpu.make_async_copy(st2(slot, k, 0, share), a.at[:, part], s2sem.at[slot, k]) for k, a in enumerate((to_r, to_l))]

    def own_copy(t):
        slot = lax.rem(t, 2)
        return pltpu.make_async_copy(sto(slot), own.at[:, pl.ds(pl.multiple_of(t * nt, nt), nt)], owsem.at[slot])

    def free_slots(p):
        @pl.when(p >= SENDS)
        def _():
            for k in (0, 1):
                t_hop(p - SENDS, k, True).wait_send()

        @pl.when(p >= KEEP)
        def _():
            for c in s2_copies(p - KEEP):
                c.wait()

        @pl.when(p >= 2)
        def _():
            own_copy(p - 2).wait()

    def strips(slot, hold, out):
        def term(device, start, size):
            return res(slot)[rows_of(device, share, start, size), :]

        rsend[out, 0] = term(opposite, 0, half).astype(BF16)
        rsend[out, 1] = term(opposite, half, half).astype(BF16)
        keep(hold, 0)[...] = term(right, 0, half)
        keep(hold, 1)[...] = term(left, half, half)
        st2(hold, 0, half, half)[...] = term(right, half, half).astype(BF16)
        st2(hold, 1, 0, half)[...] = term(left, 0, half).astype(BF16)
        sto(slot)[...] = term(me, 0, share)

    def arrive(u):
        hold = lax.rem(u, KEEP)
        for k in (0, 1):
            t_hop(u, k, False).wait_recv()
        st2(hold, 0, 0, half)[...] = (keep(hold, 0)[...] + rrecv[u, 0].astype(F32)).astype(BF16)
        st2(hold, 1, half, half)[...] = (keep(hold, 1)[...] + rrecv[u, 1].astype(F32)).astype(BF16)
        for c in s2_copies(u):
            c.start()

    for s in (total - 2, total - 1):
        for c in o_copies(s):
            c.wait()

    def dx_step(t, _):
        @pl.when(t >= 2)
        def _():
            for k in (0, 1):
                t_hop(t - 2, k, True).start()

        @pl.when(jnp.logical_and(lax.rem(t, 4) == 0, t < 2 * chunks))
        def _():
            x_pass(t // 4)

        @pl.when(jnp.logical_and(lax.rem(t, 4) == 2, t < 2 * chunks))
        def _():
            x_own(chunks // 2 + t // 4)

        @pl.when(t >= DELAY)
        def _():
            arrive(t - DELAY)

        slot = lax.rem(t, 2)
        for c in w2_copies(t):
            c.wait()

        @pl.when(t + 1 < tiles)
        def _():
            for c in w2_copies(t + 1):
                c.start()

        free_slots(t - 1)
        res(slot)[...] = dot_nt(dgv[...], w2[slot, 0]) + dot_nt(duv[...], w2[slot, 1])
        strips(1 - slot, lax.rem(t + KEEP - 1, KEEP), lax.rem(t + SENDS - 1, SENDS))

        @pl.when(t >= 1)
        def _():
            own_copy(t - 1).start()

        return 0

    lax.fori_loop(0, tiles, dx_step, 0)
    last = tiles - 1
    for k in (0, 1):
        t_hop(last - 1, k, True).start()
    free_slots(last)
    strips(last % 2, last % KEEP, last % SENDS)
    own_copy(last).start()
    for k in (0, 1):
        t_hop(last, k, True).start()

    def late(u, _):
        arrive(u)
        return 0

    lax.fori_loop(tiles - DELAY, tiles, late, 0)
    for c in d_copies:
        c.wait()
    x_local.wait()
    for t in range(tiles - 2, tiles):
        own_copy(t).wait()
    for t in range(tiles - KEEP, tiles):
        for c in s2_copies(t):
            c.wait()
    for t in range(tiles - SENDS, tiles):
        for k in (0, 1):
            t_hop(t, k, True).wait_send()

    def finish_dy(j, _):
        for kind in range(6):
            hop(kind, j, True).wait_send()
        return 0

    lax.fori_loop(0, blocks, finish_dy, 0)

    def finish_first(c, _):
        xhop(1, c, False).wait_recv()
        xhop(2, c, False).wait_recv()
        xhop(2, c, True).wait_send()
        for kind in (0, 1):
            xhop(kind, c, True).wait_send()
        return 0

    def finish_second(c, _):
        xhop(0, c, False).wait_recv()
        xhop(3, c, False).wait_recv()
        xhop(3, c, True).wait_send()
        for kind in (0, 1):
            xhop(kind, c, True).wait_send()
        return 0

    lax.fori_loop(0, chunks // 2, finish_first, 0)
    lax.fori_loop(chunks // 2, chunks, finish_second, 0)


def dw_kernel(xf, dg, du, ready, dwg, dwu, copied, cbuf, isem, osem):
    i = pl.program_id(0)
    steps = pl.num_programs(0)
    size = cbuf.shape[1]

    def copies(c):
        slot = lax.rem(c, 2)
        part = pl.ds(pl.multiple_of(c * size, size), size)
        return (
            pltpu.make_async_copy(ready.at[part, :], cbuf.at[slot], isem.at[slot]),
            pltpu.make_async_copy(cbuf.at[slot], copied.at[part, :], osem.at[slot]),
        )

    @pl.when(lax.rem(i, 2) == 0)
    def _():
        @pl.when(i >= 4)
        def _():
            copies(i // 2 - 2)[1].wait()

        copies(i // 2)[0].start()

    @pl.when(lax.rem(i, 2) == 1)
    def _():
        copies(i // 2)[0].wait()
        copies(i // 2)[1].start()

    t = xf[...]
    dwg[...] = dot_tn(t, dg[...]).astype(BF16)
    dwu[...] = dot_tn(t, du[...]).astype(BF16)

    @pl.when(i == steps - 1)
    def _():
        copies(steps // 2 - 2)[1].wait()
        copies(steps // 2 - 1)[1].wait()


def cost(flops, nbytes):
    return pl.CostEstimate(flops=flops, bytes_accessed=nbytes, transcendentals=0)


def solution(mesh):
    n = mesh.shape["tp"]

    def body(x, dy, gate, up, w_gate, w_up, w_down):
        share, width = x.shape
        rows, ff = gate.shape
        blocks, tiles, half = width // CB, width // NT, share // 2
        any_, vmem, dma = pl.BlockSpec(memory_space=pl.ANY), pltpu.VMEM, pltpu.SemaphoreType.DMA
        flops = 2 * rows * width * ff
        act, wbytes = rows * ff * 2, width * ff * 2
        shape = jax.ShapeDtypeStruct

        dg, du, dwd, xf, to_r, to_l, own = pl.pallas_call(
            functools.partial(main_kernel, n),
            out_shape=[
                shape((rows, ff), BF16),
                shape((rows, ff), BF16),
                shape((ff, width), BF16),
                shape((rows, width), BF16),
                shape((share, width), BF16),
                shape((share, width), BF16),
                shape((share, width), F32),
            ],
            in_specs=[any_] * 7,
            out_specs=[any_] * 7,
            scratch_shapes=[
                vmem((blocks, rows, CB), BF16),
                vmem((ff, rows), BF16),
                vmem((ff // ET, rows, ET), F32),
                vmem((rows, ff), BF16),
                vmem((rows, ff), BF16),
                vmem((2, FT, CB), BF16),
                vmem((2, 2, rows, ET), BF16),
                vmem((2, 2, NT, ff), BF16),
                vmem((SENDS, 2, half, NT), BF16),
                vmem((tiles, 2, half, NT), BF16),
                dma((blocks,)),
                dma((6, blocks)),
                dma((6, blocks)),
                dma((2,)),
                dma((2, FT // NT)),
                dma((2, 2)),
                dma((3,)),
                dma((2, 2)),
                dma((4, share // XR)),
                dma((4, share // XR)),
                dma((SENDS, 2)),
                dma((tiles, 2)),
                dma((KEEP, 2)),
                dma((2,)),
            ],
            compiler_params=pltpu.CompilerParams(collective_id=0, has_side_effects=True, vmem_limit_bytes=VMEM_LIMIT),
            cost_estimate=cost(4 * flops, 4 * wbytes + 8 * act),
            name="dhidden_dwdown_dx",
        )(dy, gate, up, w_down, w_gate, w_up, x)

        from_l = lax.ppermute(to_r, "tp", [(i, (i + 1) % n) for i in range(n)])
        from_r = lax.ppermute(to_l, "tp", [(i, (i - 1) % n) for i in range(n)])

        whole = pl.BlockSpec((rows, ff), lambda i: (0, 0), pipeline_mode=pl.Buffered(1))
        out_spec = pl.BlockSpec((DT, ff), lambda i: (i, 0))
        dwg, dwu, dwd = pl.pallas_call(
            dw_kernel,
            grid=(width // DT,),
            out_shape=[shape((width, ff), BF16), shape((width, ff), BF16), shape((ff, width), BF16)],
            in_specs=[pl.BlockSpec((rows, DT), lambda i: (0, i)), whole, whole, any_],
            out_specs=[out_spec, out_spec, any_],
            scratch_shapes=[vmem((2, ff * DT * 2 // width, width), BF16), dma((2,)), dma((2,))],
            compiler_params=pltpu.CompilerParams(vmem_limit_bytes=55_000_000, dimension_semantics=("arbitrary",)),
            cost_estimate=cost(2 * flops, 4 * wbytes + 4 * act),
            name="dw_gate_up",
        )(xf, dg, du, dwd)

        dx = (own + from_l.astype(F32) + from_r.astype(F32)).astype(BF16)
        return dx, dwg, dwu, dwd

    part, cols = P(("dp", "tp"), None), P("dp", "tp")
    return jax.shard_map(
        body,
        mesh=mesh,
        in_specs=(part, part, cols, cols, P(None, "tp"), P(None, "tp"), P("tp", None)),
        out_specs=(part, cols, cols, part),
        check_vma=False,
    )
```
